32 devices in a mesh: ta: 4 (over y, x), gz: 2 (over core), xy: 4 (over z).
Axes of the slice: x: 2, y: 2, z: 4, core: 2. Of those that a mesh axis runs over, the one named last changes fastest.
Arguments:
- source: float32 [2, 4, 3, 16, 16, 512], P(None, None, None, 'ta', 'gz', 'xy'), may hold values from -6 to 6
- iterate: float32 [2, 4, 3, 16, 16, 512], P(None, None, None, 'ta', 'gz', 'xy'), may hold values from -6 to 6
- gauge_links: float32 [4, 2, 3, 3, 16, 16, 512], P(None, None, None, None, 'ta', 'gz', 'xy'), may hold values from -2.4 to 2.4
- clover: float32 [2, 2, 6, 6, 16, 16, 512], P(None, None, None, None, 'ta', 'gz', 'xy'), may hold values from -0.6 to 0.6
- bc_sign: int32 [4], replicated, may hold values from -1 to 1, as said below
- null_store: bfloat16 [4, 4, 4, 2, 24, 12, 4, 4, 128], P('ta', 'gz', 'xy'), may hold values from -0.109375 to 0.109375
- block_slot: int32 [4, 4, 4], P('ta', 'gz', 'xy'), may hold values from 0 to 1, as said below
- coarse_links: float32 [9, 2, 24, 24, 4, 4, 4, 8], P(None, None, None, None, 'ta', 'gz', 'xy'), may hold values from -0.2 to 0.2
Outputs:
- new_iterate: float32 [2, 4, 3, 16, 16, 512], P(None, None, None, 'ta', 'gz', 'xy')
- new_residual: float32 [2, 4, 3, 16, 16, 512], P(None, None, None, 'ta', 'gz', 'xy')
The draws below stay inside these ranges and needn't reach their ends.
Inputs may be any that keep to these rules, and one draw needn't show every extreme that they name: `bc_sign`: each entry is -1 or +1. `block_slot`: within each device's block of 2 aggregate columns the entries are the numbers 0 to 1, each once.
All inputs are finite; a program needn't handle non-finite values.
Results may differ from the reference program's by a relative error of at most 0.0016.
Values sent between devices are 32-bit elements; how exact they have to be, the bound alone decides.
No kernel may reach another device: no remote copies, remote signals or barrier semaphores. Data moves between devices by JAX's collectives and lax.ppermute only.
A program may use at most 256 MiB of HBM per device.

```python
import jax
import jax.numpy as jnp
import numpy as np
from jax import lax

NV = 24
BLK = 4
LT = 4
LZ = 8
LX = 4
LY = 32
CITERS = 4
NT = 16
NZ = 16
NXY = 512
CT = 4
CZ = 4
CX = 4
CY = 8


def draw_bc_sign(key, part):
    return 2 * jax.random.randint(key, (4,), 0, 2, dtype=jnp.int32) - 1


def draw_block_slot(key, part):
    dev_t = LT // BLK
    dev_z = LZ // BLK
    dev_x = LX // BLK
    count_t = CT // dev_t
    count_z = CZ // dev_z
    count_x = CX // dev_x
    per_device = dev_t * dev_z * dev_x
    scores = jax.random.randint(key, (count_t * count_z * count_x, per_device), 0, 1 << 16, dtype=jnp.int32)
    scores = scores * per_device + jnp.arange(per_device, dtype=jnp.int32)[None, :]
    ordering = jnp.argsort(scores, axis=1).astype(jnp.int32)
    ordering = ordering.reshape((count_t, count_z, count_x, dev_t, dev_z, dev_x))
    ordering = jnp.transpose(ordering, (0, 3, 1, 4, 2, 5))
    return ordering.reshape((CT, CZ, CX))


def level_of(own_key, shape, split, smallest, high):
    def one(dim, parts):
        draws = jax.random.uniform(jax.random.fold_in(jax.random.fold_in(own_key, 6), dim), (parts,), jnp.float32, smallest / len(split), high / len(split))
        return jnp.repeat(jnp.exp(draws), shape[dim] // parts).reshape((-1,) + (1,) * (len(shape) - dim - 1))

    loudness = one(*split[0])
    for cut in split[1:]:
        loudness = loudness * one(*cut)
    return loudness


def scatter_about(stream_key, shape, scale, bound, cuts=(), kind=jnp.bfloat16):
    values = scale * jax.random.normal(stream_key, shape, jnp.float32)
    if cuts:
        values = values * level_of(stream_key, shape, cuts, -0.22, 0.18)
    return jnp.clip(values, -bound, bound).astype(kind)


def setup_inputs(seed: int = 0) -> dict:
    key_list = jax.random.split(jax.random.key(seed), 9)
    source = scatter_about(key_list[0], (2, 4, 3, NT, NZ, NXY), 1.0, 6.0, ((3, 4), (4, 2), (5, 4)), jnp.float32)
    iterate = scatter_about(key_list[1], (2, 4, 3, NT, NZ, NXY), 1.0, 6.0, ((3, 4), (4, 2), (5, 4)), jnp.float32)
    gauge_links = scatter_about(key_list[2], (4, 2, 3, 3, NT, NZ, NXY), 0.4, 2.4, ((4, 4), (5, 2), (6, 4)), jnp.float32)
    clover = scatter_about(key_list[3], (2, 2, 6, 6, NT, NZ, NXY), 0.1, 0.6, ((4, 4), (5, 2), (6, 4)), jnp.float32)
    bc_sign = draw_bc_sign(jax.random.fold_in(key_list[8], 71), 0)
    null_store = scatter_about(key_list[5], (CT, CZ, CX, 2, NV, 12, BLK, BLK, BLK * LY), (12 * BLK ** 4) ** -0.5, 0.109375, ((0, 4), (1, 2), (2, 4)))
    block_slot = draw_block_slot(jax.random.fold_in(key_list[8], 71), 0)
    coarse_links = scatter_about(key_list[7], (9, 2, NV, NV, CT, CZ, CX, CY), 0.03, 0.2, ((4, 4), (5, 2), (6, 4)), jnp.float32)
    return {"source": source, "iterate": iterate, "gauge_links": gauge_links, "clover": clover, "bc_sign": bc_sign, "null_store": null_store, "block_slot": block_slot, "coarse_links": coarse_links}


MASS_TERM = 3.8
RELAX_WEIGHT = 0.4
HIGHEST = lax.Precision.HIGHEST


def chiral_blocks():
    identity = np.eye(2)
    nought = np.zeros((2, 2))
    flip_x = np.array([[0.0, 1.0], [1.0, 0.0]])
    flip_z = np.array([[1.0, 0.0], [0.0, -1.0]])
    rotate = np.array([[0.0, -1.0], [1.0, 0.0]])
    return [(identity, nought), (nought, -flip_z), (nought, -flip_x), (rotate, nought)]


def four_square(top_left, top_right, bottom_left, bottom_right):
    upper = np.concatenate([top_left, top_right], axis=1)
    lower = np.concatenate([bottom_left, bottom_right], axis=1)
    return np.concatenate([upper, lower], axis=0)


def spin_tables(direction, parity):
    upper_re, upper_im = chiral_blocks()[direction]
    identity = np.eye(2)
    nought = np.zeros((2, 2))
    gamma_re = four_square(nought, upper_re, upper_re.T, nought)
    gamma_im = four_square(nought, upper_im, -upper_im.T, nought)
    whole_re = np.eye(4) + parity * gamma_re
    whole_im = parity * gamma_im
    half_re = np.concatenate([identity, parity * upper_re], axis=1)
    half_im = np.concatenate([nought, parity * upper_im], axis=1)
    back_re = np.concatenate([identity, parity * upper_re.T], axis=0)
    back_im = np.concatenate([nought, -parity * upper_im.T], axis=0)
    return [np.asarray(matrix, np.float32) for matrix in (whole_re, whole_im, half_re, half_im, back_re, back_im)]


def spin_times(matrix_re, matrix_im, field):
    real_part = jnp.tensordot(matrix_re, field[0], axes=(1, 0), precision=HIGHEST) - jnp.tensordot(matrix_im, field[1], axes=(1, 0), precision=HIGHEST)
    imag_part = jnp.tensordot(matrix_re, field[1], axes=(1, 0), precision=HIGHEST) + jnp.tensordot(matrix_im, field[0], axes=(1, 0), precision=HIGHEST)
    return jnp.stack([real_part, imag_part])


def colour_times(link, field):
    real_part = 0.0
    imag_part = 0.0
    for column in range(3):
        link_re = link[0][:, column][None]
        link_im = link[1][:, column][None]
        field_re = field[0][:, column:column + 1]
        field_im = field[1][:, column:column + 1]
        real_part = real_part + link_re * field_re - link_im * field_im
        imag_part = imag_part + link_re * field_im + link_im * field_re
    return jnp.stack([real_part, imag_part])


def colour_dagger(link, field):
    real_part = 0.0
    imag_part = 0.0
    for column in range(3):
        link_re = link[0][column][None]
        link_im = link[1][column][None]
        field_re = field[0][:, column:column + 1]
        field_im = field[1][:, column:column + 1]
        real_part = real_part + link_re * field_re + link_im * field_im
        imag_part = imag_part + link_re * field_im - link_im * field_re
    return jnp.stack([real_part, imag_part])


def clover_times(clover, field):
    halves = []
    for chirality in range(2):
        chiral_part = field[:, 2 * chirality:2 * chirality + 2]
        chiral_part = chiral_part.reshape((2, 6) + chiral_part.shape[3:])
        matrix_re = clover[chirality, 0]
        matrix_im = clover[chirality, 1]
        real_part = 0.0
        imag_part = 0.0
        for column in range(6):
            real_part = real_part + matrix_re[:, column] * chiral_part[0, column][None] - matrix_im[:, column] * chiral_part[1, column][None]
            imag_part = imag_part + matrix_re[:, column] * chiral_part[1, column][None] + matrix_im[:, column] * chiral_part[0, column][None]
        halves.append(jnp.stack([real_part, imag_part]).reshape((2, 2, 3) + chiral_part.shape[2:]))
    return jnp.concatenate(halves, axis=1)


def along_y(field, forward):
    column_y = jnp.arange(field.shape[-1], dtype=jnp.int32) % LY
    if forward:
        return jnp.where(column_y == LY - 1, jnp.roll(field, LY - 1, axis=-1), jnp.roll(field, -1, axis=-1))
    return jnp.where(column_y == 0, jnp.roll(field, 1 - LY, axis=-1), jnp.roll(field, 1, axis=-1))


def neighbour(field, direction, forward):
    offset = -1 if forward else 1
    if direction == 0:
        return jnp.roll(field, offset, axis=-3)
    if direction == 1:
        return jnp.roll(field, offset, axis=-2)
    if direction == 2:
        return jnp.roll(field, offset * LY, axis=-1)
    return along_y(field, forward)


def edge_factors(bc_sign, shape):
    count_t, count_z, count_xy = shape
    flat_index = jnp.arange(count_xy, dtype=jnp.int32)
    places = [(jnp.arange(count_t, dtype=jnp.int32)[:, None, None], count_t),
              (jnp.arange(count_z, dtype=jnp.int32)[None, :, None], count_z),
              ((flat_index // LY)[None, None, :], count_xy // LY),
              ((flat_index % LY)[None, None, :], LY)]
    factors = []
    for direction in range(4):
        where_now, extent = places[direction]
        flipped = bc_sign[direction].astype(jnp.float32)
        factors.append((jnp.where(where_now == extent - 1, flipped, 1.0), jnp.where(where_now == 0, flipped, 1.0)))
    return factors


def fine_apply(field, gauge_links, clover, factors):
    result = MASS_TERM * field + clover_times(clover, field)
    for direction in range(4):
        minus_tables = spin_tables(direction, -1)
        plus_tables = spin_tables(direction, 1)
        ahead = colour_times(gauge_links[direction], neighbour(field, direction, True) * factors[direction][0])
        behind = colour_dagger(neighbour(gauge_links[direction], direction, False), neighbour(field, direction, False) * factors[direction][1])
        result = result - 0.5 * (spin_times(minus_tables[0], minus_tables[1], ahead) + spin_times(plus_tables[0], plus_tables[1], behind))
    return result


def source_index(block_slot):
    dev_t, dev_z, dev_x = LT // BLK, LZ // BLK, LX // BLK
    count_t, count_z, count_x = block_slot.shape
    base_t = jnp.arange(count_t, dtype=jnp.int32)[:, None, None] // dev_t * dev_t
    base_z = jnp.arange(count_z, dtype=jnp.int32)[None, :, None] // dev_z * dev_z
    base_x = jnp.arange(count_x, dtype=jnp.int32)[None, None, :] // dev_x * dev_x
    slot_t = block_slot // (dev_z * dev_x)
    slot_z = block_slot // dev_x % dev_z
    slot_x = block_slot % dev_x
    return (((base_t + slot_t) * count_z + base_z + slot_z) * count_x + base_x + slot_x).astype(jnp.int32)


def column_layout(field):
    width = BLK * LY
    shaped = field.reshape((2, 12, CT, BLK, CZ, BLK, CX, width))
    return jnp.moveaxis(shaped, 2, 0)


def restrict_all(rounded, null_store, indices):
    columns = column_layout(rounded)
    flat_store = null_store.reshape((-1,) + null_store.shape[3:])

    def one_slice(inputs):
        field_part, index_part = inputs
        null_rows = jnp.take(flat_store, index_part.reshape(-1), axis=0).astype(jnp.float32)
        null_rows = null_rows.reshape((CZ, CX) + null_rows.shape[1:])
        field_part = field_part.astype(jnp.float32)
        turned = jnp.stack([field_part[1], -field_part[0]])
        paired = jnp.stack([field_part, turned])
        return jnp.einsum('zxpvsabw,qpsazbxw->qvzxw', null_rows, paired, precision=HIGHEST)

    coarse = lax.map(one_slice, (columns, indices))
    coarse = coarse.reshape(coarse.shape[:5] + (BLK, CY, BLK)).sum(axis=(5, 7))
    return jnp.transpose(coarse, (1, 2, 0, 3, 4, 5))


def prolong_all(coarse_round, null_store, indices):
    width = BLK * LY
    per_slice = jnp.moveaxis(coarse_round, 2, 0)
    flat_store = null_store.reshape((-1,) + null_store.shape[3:])

    def one_slice(inputs):
        coarse_part, index_part = inputs
        null_rows = jnp.take(flat_store, index_part.reshape(-1), axis=0).astype(jnp.float32)
        null_rows = null_rows.reshape((CZ, CX) + null_rows.shape[1:])
        coarse_part = coarse_part.astype(jnp.float32)
        spread = jnp.broadcast_to(coarse_part[..., None, :, None], coarse_part.shape[:4] + (BLK, CY, BLK))
        spread = spread.reshape(coarse_part.shape[:4] + (width,))
        mixture = jnp.stack([jnp.stack([spread[0], -spread[1]]), jnp.stack([spread[1], spread[0]])])
        return jnp.einsum('zxpvsabw,qpvzxw->qsazbxw', null_rows, mixture, precision=HIGHEST)

    fine = lax.map(one_slice, (per_slice, indices))
    fine = jnp.moveaxis(fine, 0, 2)
    return fine.reshape((2, 4, 3, CT * BLK, CZ * BLK, CX * width))


def block_times(block_links, stacked):
    links_re = block_links[:, 0]
    links_im = block_links[:, 1]
    vector_re = stacked[:, 0]
    vector_im = stacked[:, 1]
    real_part = jnp.einsum('kijabcd,kjabcd->iabcd', links_re, vector_re, precision=HIGHEST) - jnp.einsum('kijabcd,kjabcd->iabcd', links_im, vector_im, precision=HIGHEST)
    imag_part = jnp.einsum('kijabcd,kjabcd->iabcd', links_re, vector_im, precision=HIGHEST) + jnp.einsum('kijabcd,kjabcd->iabcd', links_im, vector_re, precision=HIGHEST)
    return jnp.stack([real_part, imag_part])


def coarse_apply(vector, coarse_links):
    neighbours = [vector,
                  jnp.roll(vector, -1, 2), jnp.roll(vector, 1, 2),
                  jnp.roll(vector, -1, 3), jnp.roll(vector, 1, 3),
                  jnp.roll(vector, -1, 4), jnp.roll(vector, 1, 4),
                  jnp.roll(vector, -1, 5), jnp.roll(vector, 1, 5)]
    return 2.0 * vector + block_times(coarse_links, jnp.stack(neighbours))


def reference(source, iterate, gauge_links, clover, bc_sign, null_store, block_slot, coarse_links):
    factors = edge_factors(bc_sign, source.shape[3:])
    residual_start = source - fine_apply(iterate, gauge_links, clover, factors)
    indices = source_index(block_slot)
    coarse_rhs = restrict_all(residual_start.astype(jnp.bfloat16), null_store, indices)
    coarse_sol = RELAX_WEIGHT * coarse_rhs
    for iteration in range(CITERS - 1):
        coarse_sol = coarse_sol + RELAX_WEIGHT * (coarse_rhs - coarse_apply(coarse_sol, coarse_links))
    correction = prolong_all(coarse_sol.astype(jnp.bfloat16), null_store, indices)
    new_iterate = iterate + correction
    new_residual = residual_start - fine_apply(correction, gauge_links, clover, factors)
    return new_iterate, new_residual
```

```python
import jax
import jax.numpy as jnp
from jax import lax
from jax.experimental import pallas as pl
from jax.experimental.pallas import tpu as pltpu
from jax.sharding import PartitionSpec as P

BLK = 4
LY = 32
CITERS = 4
MASS_TERM = 3.8
RELAX_WEIGHT = 0.4
HIGHEST = lax.Precision.HIGHEST
F32 = jnp.float32
VMEM = pltpu.MemorySpace.VMEM
SMEM = pltpu.MemorySpace.SMEM


def times_i(z, sign):
    return (-z[1], z[0]) if sign > 0 else (z[1], -z[0])


def add(a, b):
    return (a[0] + b[0], a[1] + b[1])


def neg(a):
    return (-a[0], -a[1])


def upper_of(mu, low):
    if mu == 0:
        return [low[0], low[1]]
    if mu == 1:
        return [times_i(low[0], -1), times_i(low[1], 1)]
    if mu == 2:
        return [times_i(low[1], -1), times_i(low[0], -1)]
    return [neg(low[1]), low[0]]


def lower_of(mu, half):
    if mu == 0:
        return [half[0], half[1]]
    if mu == 1:
        return [times_i(half[0], 1), times_i(half[1], -1)]
    if mu == 2:
        return [times_i(half[1], 1), times_i(half[0], 1)]
    return [half[1], neg(half[0])]


def project(mu, sign, v):
    out = []
    for c in range(3):
        up = upper_of(mu, [v[2][c], v[3][c]])
        out.append([add(v[s][c], up[s] if sign > 0 else neg(up[s])) for s in range(2)])
    return [[out[c][s] for c in range(3)] for s in range(2)]


def reconstruct(mu, sign, half):
    low = [[None] * 3, [None] * 3]
    for c in range(3):
        lo = lower_of(mu, [half[0][c], half[1][c]])
        for s in range(2):
            low[s][c] = lo[s] if sign > 0 else neg(lo[s])
    return [half[0], half[1], low[0], low[1]]


def link_times(u, half):
    out = []
    for s in range(2):
        row = []
        for a in range(3):
            re = im = None
            for b in range(3):
                ur, ui = u[a][b]
                hr, hi = half[s][b]
                pr = ur * hr - ui * hi
                pi = ur * hi + ui * hr
                re = pr if re is None else re + pr
                im = pi if im is None else im + pi
            row.append((re, im))
        out.append(row)
    return out


def link_dagger(u, half):
    out = []
    for s in range(2):
        row = []
        for a in range(3):
            re = im = None
            for b in range(3):
                ur, ui = u[b][a]
                hr, hi = half[s][b]
                pr = ur * hr + ui * hi
                pi = ur * hi - ui * hr
                re = pr if re is None else re + pr
                im = pi if im is None else im + pi
            row.append((re, im))
        out.append(row)
    return out


def map_half(fn, half):
    return [[(fn(z[0]), fn(z[1])) for z in row] for row in half]


def spinor(get):
    return [[(get(0, s, c), get(1, s, c)) for c in range(3)] for s in range(4)]


def links(get):
    return [[(get(0, a, b), get(1, a, b)) for b in range(3)] for a in range(3)]


def half_of(get):
    return [[(get(0, s, c), get(1, s, c)) for c in range(3)] for s in range(2)]


def put_half(ref, half):
    for s in range(2):
        for c in range(3):
            for r in range(2):
                ref[r, s, c] = half[s][c][r]


def lane_index(shape):
    return lax.broadcasted_iota(jnp.int32, shape, len(shape) - 1)


def write_faces(field, gauge, signs, outs):
    to_down_t, to_up_t, to_down_z, to_up_z, to_down_x, to_up_x = outs
    nt, nz, nxy = field.shape[3:]
    half = project(0, -1, spinor(lambda r, s, c: field[r, s, c, 0]))
    put_half(to_down_t, map_half(lambda x: x * signs[0], half))
    half = project(0, 1, spinor(lambda r, s, c: field[r, s, c, nt - 1]))
    half = link_dagger(links(lambda r, a, b: gauge[0, r, a, b, nt - 1]), half)
    put_half(to_up_t, map_half(lambda x: x * signs[1], half))
    half = project(1, -1, spinor(lambda r, s, c: field[r, s, c, :, 0, :]))
    put_half(to_down_z, map_half(lambda x: x * signs[2], half))
    half = project(1, 1, spinor(lambda r, s, c: field[r, s, c, :, nz - 1, :]))
    half = link_dagger(links(lambda r, a, b: gauge[1, r, a, b, :, nz - 1, :]), half)
    put_half(to_up_z, map_half(lambda x: x * signs[3], half))
    lane = lane_index((nz, nxy))

    def packed(rows, first):
        out = None
        for t in range(nt):
            shift = (LY * t - first) % nxy
            x = rows(t)
            x = pltpu.roll(x, shift, 1) if shift else x
            out = x if out is None else jnp.where(lane >= LY * t, x, out)
        return out

    half = project(2, -1, spinor(lambda r, s, c: packed(lambda t: field[r, s, c, t], 0)))
    put_half(to_down_x, map_half(lambda x: x * signs[4], half))
    last = nxy - LY
    half = project(2, 1, spinor(lambda r, s, c: packed(lambda t: field[r, s, c, t], last)))
    half = link_dagger(
        links(lambda r, a, b: packed(lambda t: gauge[2, r, a, b, t], last)), half
    )
    put_half(to_up_x, map_half(lambda x: x * signs[5], half))


def add_halo(res, gauge, halos):
    from_up_t, from_down_t, from_up_z, from_down_z, from_up_x, from_down_x = halos
    nt, nz, nxy = res.shape[3:]

    def accumulate(full, index):
        for s in range(4):
            for c in range(3):
                for r in range(2):
                    where = (r, s, c) + index
                    res[where] = res[where] + 0.5 * full[s][c][r]

    half = half_of(lambda r, s, c: from_up_t[r, s, c])
    half = link_times(links(lambda r, a, b: gauge[0, r, a, b, nt - 1]), half)
    accumulate(reconstruct(0, -1, half), (nt - 1,))
    half = half_of(lambda r, s, c: from_down_t[r, s, c])
    accumulate(reconstruct(0, 1, half), (0,))
    every = slice(None)
    half = half_of(lambda r, s, c: from_up_z[r, s, c])
    half = link_times(links(lambda r, a, b: gauge[1, r, a, b, :, nz - 1, :]), half)
    accumulate(reconstruct(1, -1, half), (every, nz - 1, every))
    half = half_of(lambda r, s, c: from_down_z[r, s, c])
    accumulate(reconstruct(1, 1, half), (every, 0, every))
    lane = lane_index((nz, nxy))
    last = nxy - LY
    for t in range(nt):

        def unpacked(x, first):
            shift = (first - LY * t) % nxy
            x = pltpu.roll(x, shift, 1) if shift else x
            return jnp.where((lane >= first) & (lane < first + LY), x, 0.0)

        half = half_of(lambda r, s, c: unpacked(from_up_x[r, s, c], last))
        half = link_times(links(lambda r, a, b: gauge[2, r, a, b, t]), half)
        accumulate(reconstruct(2, -1, half), (t,))
        half = half_of(lambda r, s, c: unpacked(from_down_x[r, s, c], 0))
        accumulate(reconstruct(2, 1, half), (t,))


def local_kernel(signs, base, field, gauge, gauge_before, clover, out):
    t = pl.program_id(0)
    nt, nz, nxy = field.shape[3:]
    lane = lane_index((nz, nxy))
    depth = lax.broadcasted_iota(jnp.int32, (nz, nxy), 0)
    y = lane % LY
    v = spinor(lambda r, s, c: field[r, s, c, t])
    hops = [[[None, None] for _ in range(3)] for _ in range(4)]

    def gather(full):
        for s in range(4):
            for c in range(3):
                for r in range(2):
                    old = hops[s][c][r]
                    hops[s][c][r] = full[s][c][r] if old is None else old + full[s][c][r]

    up = jnp.minimum(t + 1, nt - 1)
    down = jnp.maximum(t - 1, 0)
    keep_up = jnp.where(t < nt - 1, 1.0, 0.0).astype(F32)
    keep_down = jnp.where(t > 0, 1.0, 0.0).astype(F32)
    half = project(0, -1, spinor(lambda r, s, c: field[r, s, c, up]))
    half = map_half(lambda x: x * keep_up, half)
    half = link_times(links(lambda r, a, b: gauge[0, r, a, b, 0]), half)
    gather(reconstruct(0, -1, half))
    half = project(0, 1, spinor(lambda r, s, c: field[r, s, c, down]))
    half = map_half(lambda x: x * keep_down, half)
    half = link_dagger(links(lambda r, a, b: gauge_before[0, r, a, b, 0]), half)
    gather(reconstruct(0, 1, half))

    sign_y = signs[6]
    ahead_y = jnp.where(y == LY - 1, sign_y, 1.0)
    behind_y = jnp.where(y == 0, sign_y, 1.0)
    shifts = {
        1: (
            lambda x: jnp.where(depth < nz - 1, pltpu.roll(x, nz - 1, 0), 0.0),
            lambda x: jnp.where(depth > 0, pltpu.roll(x, 1, 0), 0.0),
        ),
        2: (
            lambda x: jnp.where(lane < nxy - LY, pltpu.roll(x, nxy - LY, 1), 0.0),
            lambda x: jnp.where(lane >= LY, pltpu.roll(x, LY, 1), 0.0),
        ),
        3: (
            lambda x: ahead_y
            * jnp.where(y == LY - 1, pltpu.roll(x, LY - 1, 1), pltpu.roll(x, nxy - 1, 1)),
            lambda x: behind_y
            * jnp.where(y == 0, pltpu.roll(x, nxy + 1 - LY, 1), pltpu.roll(x, 1, 1)),
        ),
    }
    for mu in (1, 2, 3):
        u = links(lambda r, a, b: gauge[mu, r, a, b, 0])
        half = map_half(shifts[mu][0], project(mu, -1, v))
        gather(reconstruct(mu, -1, link_times(u, half)))
        half = map_half(shifts[mu][1], link_dagger(u, project(mu, 1, v)))
        gather(reconstruct(mu, 1, half))

    for chi in range(2):
        for a in range(6):
            s, c = 2 * chi + a // 3, a % 3
            re = MASS_TERM * v[s][c][0] - 0.5 * hops[s][c][0]
            im = MASS_TERM * v[s][c][1] - 0.5 * hops[s][c][1]
            for b in range(6):
                vr, vi = v[2 * chi + b // 3][b % 3]
                cr = clover[chi, 0, a, b, 0]
                ci = clover[chi, 1, a, b, 0]
                re = re + cr * vr - ci * vi
                im = im + cr * vi + ci * vr
            out[0, s, c, 0] = base[0, s, c, 0] - re
            out[1, s, c, 0] = base[1, s, c, 0] - im


def apply_local(signs, base, field, gauge, clover):
    nt, nz, nxy = field.shape[3:]
    slice_of = lambda shape: pl.BlockSpec(shape, lambda t: (0,) * (len(shape) - 3) + (t, 0, 0))
    f = (2, 4, 3, 1, nz, nxy)
    return pl.pallas_call(
        local_kernel,
        grid=(nt,),
        in_specs=[
            pl.BlockSpec(memory_space=SMEM),
            slice_of(f),
            pl.BlockSpec(field.shape, lambda t: (0,) * 6),
            slice_of((4, 2, 3, 3, 1, nz, nxy)),
            pl.BlockSpec(
                (1, 2, 3, 3, 1, nz, nxy), lambda t: (0, 0, 0, 0, jnp.maximum(t - 1, 0), 0, 0)
            ),
            slice_of((2, 2, 6, 6, 1, nz, nxy)),
        ],
        out_specs=slice_of(f),
        out_shape=jax.ShapeDtypeStruct(field.shape, F32),
        cost_estimate=pl.CostEstimate(flops=12_000_000, transcendentals=0, bytes_accessed=5_000_000),
        name="local_part",
    )(signs, base, field, gauge, gauge, clover)


def face_shapes(field):
    nt, nz, nxy = field.shape[3:]
    row = jax.ShapeDtypeStruct((2, 2, 3, nz, nxy), F32)
    slab = jax.ShapeDtypeStruct((2, 2, 3, nt, nxy), F32)
    return [row, row, slab, slab, row, row]


def faces_kernel(signs, field, gauge, *outs):
    write_faces(field, gauge, signs, outs)


def whole(x):
    n = len(x.shape)
    return pl.BlockSpec(x.shape, lambda *_: (0,) * n)


def gauge_spec(gauge):
    shape = (3,) + gauge.shape[1:]
    return pl.BlockSpec(shape, lambda *_: (0,) * len(shape))


def make_faces(signs, field, gauge):
    shapes = face_shapes(field)
    return pl.pallas_call(
        faces_kernel,
        grid=(1,),
        in_specs=[pl.BlockSpec(memory_space=SMEM), whole(field), gauge_spec(gauge)],
        out_specs=[whole(s) for s in shapes],
        out_shape=shapes,
        name="faces",
    )(signs, field, gauge)


def shifted(value, axis, by):
    n = lax.axis_size(axis)
    return lax.ppermute(value, axis, [(i, (i + by) % n) for i in range(n)])


def swap_faces(faces):
    out = []
    for i, axis in enumerate(("ta", "gz", "xy")):
        out.append(shifted(faces[2 * i], axis, -1))
        out.append(shifted(faces[2 * i + 1], axis, 1))
    return out


def pair_rows(null, slots, p, v, s, t):
    return jnp.concatenate(
        [null[slot, p, v, s, t].astype(F32) for slot in slots], axis=0
    )


def cy_select(nxy, cy):
    lane = lax.broadcasted_iota(jnp.int32, (cy, nxy), 1)
    row = lax.broadcasted_iota(jnp.int32, (cy, nxy), 0)
    return jnp.where((lane % LY) // BLK == row, 1.0, 0.0).astype(F32)


def restrict_kernel(slot, partial, gauge, null, h0, h1, h2, h3, h4, h5, res, rhs, first, rounded, acc):
    step = pl.program_id(0)
    nt, nz, nxy = res.shape[3:]
    chunk = null.shape[2]
    nv = acc.shape[1]
    columns, cy = rhs.shape[1:3]

    @pl.when(step == 0)
    def _():
        res[...] = partial[...]
        add_halo(res, gauge, (h0, h1, h2, h3, h4, h5))
        rounded[...] = res[...].astype(jnp.bfloat16).astype(F32)

    slots = [slot[i] for i in range(columns)]
    for v in range(chunk):
        re = jnp.zeros((nz, nxy), F32)
        im = jnp.zeros((nz, nxy), F32)
        for s in range(12):
            for t in range(nt):
                nr = pair_rows(null, slots, 0, v, s, t)
                ni = pair_rows(null, slots, 1, v, s, t)
                fr = rounded[0, s // 3, s % 3, t]
                fi = rounded[1, s // 3, s % 3, t]
                re = re + nr * fr + ni * fi
                im = im + nr * fi - ni * fr
        acc[0, step * chunk + v] = re
        acc[1, step * chunk + v] = im

    @pl.when(step == pl.num_programs(0) - 1)
    def _():
        select = cy_select(nxy, cy)
        from_row = lax.broadcasted_iota(jnp.int32, (nv * nz, nv), 0)
        to_lane = lax.broadcasted_iota(jnp.int32, (nv * nz, nv), 1)
        for r in range(2):
            rows = acc[r].reshape(nv * nz, nxy)
            summed = lax.dot_general(
                select, rows, (((1,), (1,)), ((), ())), precision=HIGHEST, preferred_element_type=F32
            )
            for col in range(columns):
                hit = (from_row // nz == to_lane) & ((from_row % nz) // BLK == col)
                out = jnp.dot(
                    summed,
                    jnp.where(hit, 1.0, 0.0).astype(F32),
                    precision=HIGHEST,
                    preferred_element_type=F32,
                )
                rhs[r, col] = out
                first[r, col] = RELAX_WEIGHT * out


CHUNK = 3


def restrict(slot, partial, gauge, null, halos):
    columns, _, nv, comps, bt, bz, nxy = null.shape
    cy = LY // BLK
    coarse = jax.ShapeDtypeStruct((2, columns, cy, nv), F32)
    return pl.pallas_call(
        restrict_kernel,
        grid=(nv // CHUNK,),
        in_specs=[
            pl.BlockSpec(memory_space=SMEM),
            whole(partial),
            gauge_spec(gauge),
            pl.BlockSpec(
                (columns, 2, CHUNK, comps, bt, bz, nxy), lambda i: (0, 0, i, 0, 0, 0, 0)
            ),
        ]
        + [whole(h) for h in halos],
        out_specs=[whole(partial), whole(coarse), whole(coarse)],
        out_shape=[jax.ShapeDtypeStruct(partial.shape, F32), coarse, coarse],
        scratch_shapes=[
            pltpu.VMEM(partial.shape, F32),
            pltpu.VMEM((2, nv) + partial.shape[4:], F32),
        ],
        name="restrict",
    )(slot, partial, gauge, null, *halos)


def relax_kernel(rhs, w, up_t, down_t, up_z, down_z, up_x, down_x, blocks, out):
    columns, cy, nv = w.shape[1:]
    row = lax.broadcasted_iota(jnp.int32, (nv, cy, nv), 0)
    lane = lax.broadcasted_iota(jnp.int32, (nv, cy, nv), 2)
    for col in range(columns):

        def ring(r, by):
            x = w[r, col]
            if by > 0:
                return jnp.concatenate([x[1:], x[:1]], axis=0)
            return jnp.concatenate([x[-1:], x[:-1]], axis=0)

        around = []
        for r in range(2):
            around.append(
                [
                    w[r, col],
                    up_t[r, col],
                    down_t[r, col],
                    w[r, col + 1] if col < columns - 1 else up_z[r, 0],
                    w[r, col - 1] if col > 0 else down_z[r, columns - 1],
                    up_x[r, col],
                    down_x[r, col],
                    ring(r, 1),
                    ring(r, -1),
                ]
            )
        re = im = None
        for k in range(9):
            br = blocks[k, 0, :, col]
            bi = blocks[k, 1, :, col]
            wr = around[0][k][None]
            wi = around[1][k][None]
            pr = br * wr - bi * wi
            pi = br * wi + bi * wr
            re = pr if re is None else re + pr
            im = pi if im is None else im + pi
        for r, part in enumerate((re, im)):
            total = jnp.sum(part, axis=2, keepdims=True)
            total = jnp.sum(jnp.where(row == lane, total, 0.0), axis=0)
            mine = w[r, col]
            out[r, col] = mine + RELAX_WEIGHT * (rhs[r, col] - (2.0 * mine + total))


def relax(rhs, w, blocks):
    up_t = shifted(w, "ta", -1)
    down_t = shifted(w, "ta", 1)
    up_z = shifted(w, "gz", -1)
    down_z = up_z if lax.axis_size("gz") == 2 else shifted(w, "gz", 1)
    up_x = shifted(w, "xy", -1)
    down_x = shifted(w, "xy", 1)
    args = (rhs, w, up_t, down_t, up_z, down_z, up_x, down_x, blocks)
    return pl.pallas_call(
        relax_kernel,
        grid=(1,),
        in_specs=[whole(a) for a in args],
        out_specs=whole(w),
        out_shape=jax.ShapeDtypeStruct(w.shape, F32),
        name="relax",
    )(*args)


def prolong_kernel(slot, signs, w, iterate, gauge, null, corr, new, o0, o1, o2, o3, o4, o5, spread):
    step = pl.program_id(0)
    nt, nz, nxy = corr.shape[3:]
    chunk = null.shape[2]
    columns, cy, nv = w.shape[1:]

    @pl.when(step == 0)
    def _():
        select = cy_select(nxy, cy)
        depth = lax.broadcasted_iota(jnp.int32, (nv, nz, nxy), 1)
        for r in range(2):
            total = None
            for col in range(columns):
                exact = w[r, col].astype(jnp.bfloat16).astype(F32)
                wide = lax.dot_general(
                    exact, select, (((0,), (0,)), ((), ())), precision=HIGHEST, preferred_element_type=F32
                )[:, None, :]
                total = wide if total is None else jnp.where(depth // BLK >= col, wide, total)
            spread[r] = total
        corr[...] = jnp.zeros(corr.shape, F32)

    slots = [slot[i] for i in range(columns)]
    for s in range(12):
        for t in range(nt):
            re = corr[0, s // 3, s % 3, t]
            im = corr[1, s // 3, s % 3, t]
            for v in range(chunk):
                nr = pair_rows(null, slots, 0, v, s, t)
                ni = pair_rows(null, slots, 1, v, s, t)
                wr = spread[0, step * chunk + v]
                wi = spread[1, step * chunk + v]
                re = re + nr * wr - ni * wi
                im = im + nr * wi + ni * wr
            corr[0, s // 3, s % 3, t] = re
            corr[1, s // 3, s % 3, t] = im

    @pl.when(step == pl.num_programs(0) - 1)
    def _():
        new[...] = iterate[...] + corr[...]
        write_faces(corr, gauge, signs, (o0, o1, o2, o3, o4, o5))


def prolong(slot, signs, w, iterate, gauge, null):
    columns, _, nv, comps, bt, bz, nxy = null.shape
    shapes = face_shapes(iterate)
    field = jax.ShapeDtypeStruct(iterate.shape, F32)
    out = pl.pallas_call(
        prolong_kernel,
        grid=(nv // CHUNK,),
        in_specs=[
            pl.BlockSpec(memory_space=SMEM),
            pl.BlockSpec(memory_space=SMEM),
            whole(w),
            whole(iterate),
            gauge_spec(gauge),
            pl.BlockSpec(
                (columns, 2, CHUNK, comps, bt, bz, nxy), lambda i: (0, 0, i, 0, 0, 0, 0)
            ),
        ],
        out_specs=[whole(field), whole(field)] + [whole(s) for s in shapes],
        out_shape=[field, field] + shapes,
        scratch_shapes=[pltpu.VMEM((2, nv) + iterate.shape[4:], F32)],
        name="prolong",
    )(slot, signs, w, iterate, gauge, null)
    return out[0], out[1], out[2:]


def finish_kernel(partial, gauge, h0, h1, h2, h3, h4, h5, res):
    res[...] = partial[...]
    add_halo(res, gauge, (h0, h1, h2, h3, h4, h5))


def finish(partial, gauge, halos):
    return pl.pallas_call(
        finish_kernel,
        grid=(1,),
        in_specs=[whole(partial), gauge_spec(gauge)] + [whole(h) for h in halos],
        out_specs=whole(partial),
        out_shape=jax.ShapeDtypeStruct(partial.shape, F32),
        name="finish",
    )(partial, gauge, *halos)


def per_device(source, iterate, gauge_links, clover, bc_sign, null_store, block_slot, coarse_links):
    signs = []
    for i, axis in enumerate(("ta", "gz", "xy")):
        place = lax.axis_index(axis)
        signs.append(jnp.where(place == 0, bc_sign[i], 1))
        signs.append(jnp.where(place == lax.axis_size(axis) - 1, bc_sign[i], 1))
    signs.append(bc_sign[3])
    signs = jnp.stack(signs).astype(F32)
    null = null_store.reshape((-1,) + null_store.shape[3:])
    slot = block_slot.reshape(-1)
    kinds, _, nv = coarse_links.shape[:3]
    blocks = jnp.transpose(coarse_links, (0, 1, 2, 4, 5, 6, 7, 3))
    blocks = blocks.reshape((kinds, 2, nv, -1) + blocks.shape[-2:])

    faces = make_faces(signs, iterate, gauge_links)
    halos = swap_faces(faces)
    partial = apply_local(signs, source, iterate, gauge_links, clover)
    residual_start, coarse_rhs, coarse_sol = restrict(slot, partial, gauge_links, null, halos)
    for _ in range(CITERS - 1):
        coarse_sol = relax(coarse_rhs, coarse_sol, blocks)
    correction, new_iterate, faces = prolong(
        slot, signs, coarse_sol, iterate, gauge_links, null
    )
    halos = swap_faces(faces)
    partial = apply_local(signs, residual_start, correction, gauge_links, clover)
    new_residual = finish(partial, gauge_links, halos)
    return (new_iterate, new_residual)


def solution(mesh):
    placed = (
        P(None, None, None, "ta", "gz", "xy"),
        P(None, None, None, "ta", "gz", "xy"),
        P(None, None, None, None, "ta", "gz", "xy"),
        P(None, None, None, None, "ta", "gz", "xy"),
        P(),
        P("ta", "gz", "xy", None, None, None, None, None, None),
        P("ta", "gz", "xy"),
        P(None, None, None, None, "ta", "gz", "xy", None),
    )
    return jax.shard_map(
        per_device,
        mesh=mesh,
        in_specs=placed,
        out_specs=(P(None, None, None, "ta", "gz", "xy"), P(None, None, None, "ta", "gz", "xy")),
        check_vma=False,
    )
```

```python
import jax
import jax.numpy as jnp
from jax import lax
from jax.experimental import pallas as pl
from jax.experimental.pallas import tpu as pltpu
from jax.sharding import PartitionSpec as P

BLK = 4
LY = 32
CITERS = 4
MASS_TERM = 3.8
RELAX_WEIGHT = 0.4
HIGHEST = lax.Precision.HIGHEST
F32 = jnp.float32
VMEM = pltpu.MemorySpace.VMEM
SMEM = pltpu.MemorySpace.SMEM


def times_i(z, sign):
    return (-z[1], z[0]) if sign > 0 else (z[1], -z[0])


def add(a, b):
    return (a[0] + b[0], a[1] + b[1])


def neg(a):
    return (-a[0], -a[1])


def upper_of(mu, low):
    if mu == 0:
        return [low[0], low[1]]
    if mu == 1:
        return [times_i(low[0], -1), times_i(low[1], 1)]
    if mu == 2:
        return [times_i(low[1], -1), times_i(low[0], -1)]
    return [neg(low[1]), low[0]]


def lower_of(mu, half):
    if mu == 0:
        return [half[0], half[1]]
    if mu == 1:
        return [times_i(half[0], 1), times_i(half[1], -1)]
    if mu == 2:
        return [times_i(half[1], 1), times_i(half[0], 1)]
    return [half[1], neg(half[0])]


def project(mu, sign, v):
    out = []
    for c in range(3):
        up = upper_of(mu, [v[2][c], v[3][c]])
        out.append([add(v[s][c], up[s] if sign > 0 else neg(up[s])) for s in range(2)])
    return [[out[c][s] for c in range(3)] for s in range(2)]


def reconstruct(mu, sign, half):
    low = [[None] * 3, [None] * 3]
    for c in range(3):
        lo = lower_of(mu, [half[0][c], half[1][c]])
        for s in range(2):
            low[s][c] = lo[s] if sign > 0 else neg(lo[s])
    return [half[0], half[1], low[0], low[1]]


def link_times(u, half):
    out = []
    for s in range(2):
        row = []
        for a in range(3):
            re = im = None
            for b in range(3):
                ur, ui = u[a][b]
                hr, hi = half[s][b]
                pr = ur * hr - ui * hi
                pi = ur * hi + ui * hr
                re = pr if re is None else re + pr
                im = pi if im is None else im + pi
            row.append((re, im))
        out.append(row)
    return out


def link_dagger(u, half):
    out = []
    for s in range(2):
        row = []
        for a in range(3):
            re = im = None
            for b in range(3):
                ur, ui = u[b][a]
                hr, hi = half[s][b]
                pr = ur * hr + ui * hi
                pi = ur * hi - ui * hr
                re = pr if re is None else re + pr
                im = pi if im is None else im + pi
            row.append((re, im))
        out.append(row)
    return out


def map_half(fn, half):
    return [[(fn(z[0]), fn(z[1])) for z in row] for row in half]


def spinor(get):
    return [[(get(0, s, c), get(1, s, c)) for c in range(3)] for s in range(4)]


def links(get):
    return [[(get(0, a, b), get(1, a, b)) for b in range(3)] for a in range(3)]


def half_of(get):
    return [[(get(0, s, c), get(1, s, c)) for c in range(3)] for s in range(2)]


def put_half(ref, half):
    for s in range(2):
        for c in range(3):
            for r in range(2):
                ref[r, s, c] = half[s][c][r]


def lane_index(shape):
    return lax.broadcasted_iota(jnp.int32, shape, len(shape) - 1)


def edge_signs(bc):
    signs = []
    for i, axis in enumerate(("ta", "gz", "xy")):
        place = lax.axis_index(axis)
        flip = bc[i].astype(F32)
        signs.append(jnp.where(place == 0, flip, 1.0))
        signs.append(jnp.where(place == lax.axis_size(axis) - 1, flip, 1.0))
    return signs


def write_faces(field, gauge, signs, outs):
    to_down_t, to_up_t, to_down_z, to_up_z, to_down_x, to_up_x = outs
    nt, nz, nxy = field.shape[3:]
    half = project(0, -1, spinor(lambda r, s, c: field[r, s, c, 0]))
    put_half(to_down_t, map_half(lambda x: x * signs[0], half))
    half = project(0, 1, spinor(lambda r, s, c: field[r, s, c, nt - 1]))
    half = link_dagger(links(lambda r, a, b: gauge[0, r, a, b, nt - 1]), half)
    put_half(to_up_t, map_half(lambda x: x * signs[1], half))
    half = project(1, -1, spinor(lambda r, s, c: field[r, s, c, :, 0, :]))
    put_half(to_down_z, map_half(lambda x: x * signs[2], half))
    half = project(1, 1, spinor(lambda r, s, c: field[r, s, c, :, nz - 1, :]))
    half = link_dagger(links(lambda r, a, b: gauge[1, r, a, b, :, nz - 1, :]), half)
    put_half(to_up_z, map_half(lambda x: x * signs[3], half))
    lane = lane_index((nz, nxy))

    def packed(rows, first):
        out = None
        for t in range(nt):
            shift = (LY * t - first) % nxy
            x = rows(t)
            x = pltpu.roll(x, shift, 1) if shift else x
            out = x if out is None else jnp.where(lane >= LY * t, x, out)
        return out

    half = project(2, -1, spinor(lambda r, s, c: packed(lambda t: field[r, s, c, t], 0)))
    put_half(to_down_x, map_half(lambda x: x * signs[4], half))
    last = nxy - LY
    half = project(2, 1, spinor(lambda r, s, c: packed(lambda t: field[r, s, c, t], last)))
    half = link_dagger(
        links(lambda r, a, b: packed(lambda t: gauge[2, r, a, b, t], last)), half
    )
    put_half(to_up_x, map_half(lambda x: x * signs[5], half))


def add_halo(res, gauge, halos):
    from_up_t, from_down_t, from_up_z, from_down_z, from_up_x, from_down_x = halos
    nt, nz, nxy = res.shape[3:]

    def accumulate(full, index):
        for s in range(4):
            for c in range(3):
                for r in range(2):
                    where = (r, s, c) + index
                    res[where] = res[where] + 0.5 * full[s][c][r]

    half = half_of(lambda r, s, c: from_up_t[r, s, c])
    half = link_times(links(lambda r, a, b: gauge[0, r, a, b, nt - 1]), half)
    accumulate(reconstruct(0, -1, half), (nt - 1,))
    half = half_of(lambda r, s, c: from_down_t[r, s, c])
    accumulate(reconstruct(0, 1, half), (0,))
    every = slice(None)
    half = half_of(lambda r, s, c: from_up_z[r, s, c])
    half = link_times(links(lambda r, a, b: gauge[1, r, a, b, :, nz - 1, :]), half)
    accumulate(reconstruct(1, -1, half), (every, nz - 1, every))
    half = half_of(lambda r, s, c: from_down_z[r, s, c])
    accumulate(reconstruct(1, 1, half), (every, 0, every))
    lane = lane_index((nz, nxy))
    last = nxy - LY
    for t in range(nt):

        def unpacked(x, first):
            shift = (first - LY * t) % nxy
            x = pltpu.roll(x, shift, 1) if shift else x
            return jnp.where((lane >= first) & (lane < first + LY), x, 0.0)

        half = half_of(lambda r, s, c: unpacked(from_up_x[r, s, c], last))
        half = link_times(links(lambda r, a, b: gauge[2, r, a, b, t]), half)
        accumulate(reconstruct(2, -1, half), (t,))
        half = half_of(lambda r, s, c: unpacked(from_down_x[r, s, c], 0))
        accumulate(reconstruct(2, 1, half), (t,))


def local_kernel(signs, base, field, gauge, clover, out):
    t = pl.program_id(0)
    nt, nz, nxy = field.shape[3:]
    lane = lane_index((nz, nxy))
    depth = lax.broadcasted_iota(jnp.int32, (nz, nxy), 0)
    y = lane % LY
    v = spinor(lambda r, s, c: field[r, s, c, t])
    hops = [[[None, None] for _ in range(3)] for _ in range(4)]

    def gather(full):
        for s in range(4):
            for c in range(3):
                for r in range(2):
                    old = hops[s][c][r]
                    hops[s][c][r] = full[s][c][r] if old is None else old + full[s][c][r]

    up = jnp.minimum(t + 1, nt - 1)
    down = jnp.maximum(t - 1, 0)
    keep_up = jnp.where(t < nt - 1, 1.0, 0.0).astype(F32)
    keep_down = jnp.where(t > 0, 1.0, 0.0).astype(F32)
    half = project(0, -1, spinor(lambda r, s, c: field[r, s, c, up]))
    half = map_half(lambda x: x * keep_up, half)
    half = link_times(links(lambda r, a, b: gauge[0, r, a, b, t]), half)
    gather(reconstruct(0, -1, half))
    half = project(0, 1, spinor(lambda r, s, c: field[r, s, c, down]))
    half = map_half(lambda x: x * keep_down, half)
    half = link_dagger(links(lambda r, a, b: gauge[0, r, a, b, down]), half)
    gather(reconstruct(0, 1, half))

    sign_y = signs[3].astype(F32)
    ahead_y = jnp.where(y == LY - 1, sign_y, 1.0)
    behind_y = jnp.where(y == 0, sign_y, 1.0)
    shifts = {
        1: (
            lambda x: jnp.where(depth < nz - 1, pltpu.roll(x, nz - 1, 0), 0.0),
            lambda x: jnp.where(depth > 0, pltpu.roll(x, 1, 0), 0.0),
        ),
        2: (
            lambda x: jnp.where(lane < nxy - LY, pltpu.roll(x, nxy - LY, 1), 0.0),
            lambda x: jnp.where(lane >= LY, pltpu.roll(x, LY, 1), 0.0),
        ),
        3: (
            lambda x: ahead_y
            * jnp.where(y == LY - 1, pltpu.roll(x, LY - 1, 1), pltpu.roll(x, nxy - 1, 1)),
            lambda x: behind_y
            * jnp.where(y == 0, pltpu.roll(x, nxy + 1 - LY, 1), pltpu.roll(x, 1, 1)),
        ),
    }
    for mu in (1, 2, 3):
        u = links(lambda r, a, b: gauge[mu, r, a, b, t])
        half = map_half(shifts[mu][0], project(mu, -1, v))
        gather(reconstruct(mu, -1, link_times(u, half)))
        half = map_half(shifts[mu][1], link_dagger(u, project(mu, 1, v)))
        gather(reconstruct(mu, 1, half))

    for chi in range(2):
        for a in range(6):
            s, c = 2 * chi + a // 3, a % 3
            re = MASS_TERM * v[s][c][0] - 0.5 * hops[s][c][0]
            im = MASS_TERM * v[s][c][1] - 0.5 * hops[s][c][1]
            for b in range(6):
                vr, vi = v[2 * chi + b // 3][b % 3]
                cr = clover[chi, 0, a, b, t]
                ci = clover[chi, 1, a, b, t]
                re = re + cr * vr - ci * vi
                im = im + cr * vi + ci * vr
            out[0, s, c, t] = base[0, s, c, t] - re
            out[1, s, c, t] = base[1, s, c, t] - im


def apply_local(signs, base, field, gauge, clover):
    return pl.pallas_call(
        local_kernel,
        grid=(field.shape[3],),
        in_specs=[pl.BlockSpec(memory_space=SMEM)] + [whole(None)] * 4,
        out_specs=whole(None),
        out_shape=near_like(field.shape),
        cost_estimate=pl.CostEstimate(flops=12_000_000, transcendentals=0, bytes_accessed=5_000_000),
        name="local_part",
        compiler_params=pltpu.CompilerParams(vmem_limit_bytes=24 << 20),
    )(signs, near(base), near(field), near(gauge), near(clover))


def face_shapes(field):
    nt, nz, nxy = field.shape[3:]
    row = near_like((2, 2, 3, nz, nxy))
    slab = near_like((2, 2, 3, nt, nxy))
    return [row, row, slab, slab, row, row]


def faces_kernel(signs, field, gauge, *outs):
    write_faces(field, gauge, edge_signs(signs), outs)


def whole(x):
    return pl.BlockSpec(memory_space=VMEM)


def gauge_spec(gauge):
    return whole(gauge)


def full_block(x):
    n = len(x.shape)
    return pl.BlockSpec(x.shape, lambda *_: (0,) * n)


def near(x):
    return pltpu.with_memory_space_constraint(x, VMEM)


def near_like(shape):
    return VMEM(tuple(shape), F32)


def make_faces(signs, field, gauge):
    shapes = face_shapes(field)
    return pl.pallas_call(
        faces_kernel,
        grid=(1,),
        in_specs=[pl.BlockSpec(memory_space=SMEM), whole(field), gauge_spec(gauge)],
        out_specs=[whole(s) for s in shapes],
        out_shape=shapes,
        name="faces",
        compiler_params=pltpu.CompilerParams(vmem_limit_bytes=24 << 20),
    )(signs, near(field), near(gauge))


def shifted(value, axis, by):
    n = lax.axis_size(axis)
    return lax.ppermute(value, axis, [(i, (i + by) % n) for i in range(n)])


def swap_faces(faces):
    out = []
    for i, axis in enumerate(("ta", "gz", "xy")):
        out.append(shifted(faces[2 * i], axis, -1))
        out.append(shifted(faces[2 * i + 1], axis, 1))
    return out


def cy_select(nxy, cy):
    lane = lax.broadcasted_iota(jnp.int32, (cy, nxy), 1)
    row = lax.broadcasted_iota(jnp.int32, (cy, nxy), 0)
    return jnp.where((lane % LY) // BLK == row, 1.0, 0.0).astype(F32)


def restrict_kernel(slot, partial, gauge, null, h0, h1, h2, h3, h4, h5, res, rhs, first, rounded, acc):
    step = pl.program_id(0)
    nt, nz, nxy = res.shape[3:]
    chunk = null.shape[2]
    nv = acc.shape[2]
    columns, cy = rhs.shape[1:3]

    rows = nt * BLK

    @pl.when(step == 0)
    def _():
        res[...] = partial[...]
        add_halo(res, gauge, (h0, h1, h2, h3, h4, h5))
        for r in range(2):
            for s in range(12):
                for col in range(columns):
                    parts = [
                        res[r, s // 3, s % 3, t, col * BLK : (col + 1) * BLK] for t in range(nt)
                    ]
                    part = jnp.concatenate(parts, axis=0)
                    rounded[col, r, s] = part.astype(jnp.bfloat16).astype(F32)

    for col in range(columns):
        here = slot[col]
        res_re = [jnp.zeros((rows, nxy), F32) for _ in range(chunk)]
        res_im = [jnp.zeros((rows, nxy), F32) for _ in range(chunk)]
        for s in range(12):
            fr = rounded[col, 0, s]
            fi = rounded[col, 1, s]
            for v in range(chunk):
                nr = null[here, 0, v, s].astype(F32)
                ni = null[here, 1, v, s].astype(F32)
                res_re[v] = res_re[v] + nr * fr + ni * fi
                res_im[v] = res_im[v] + nr * fi - ni * fr
        for v in range(chunk):
            for r, part in enumerate((res_re[v], res_im[v])):
                total = part[0:8]
                for first_row in range(8, rows, 8):
                    total = total + part[first_row : first_row + 8]
                acc[r, col, step * chunk + v] = total

    @pl.when(step == pl.num_programs(0) - 1)
    def _():
        select = cy_select(nxy, cy)
        from_row = lax.broadcasted_iota(jnp.int32, (nv * 8, nv), 0)
        to_lane = lax.broadcasted_iota(jnp.int32, (nv * 8, nv), 1)
        hit = jnp.where(from_row // 8 == to_lane, 1.0, 0.0).astype(F32)
        for r in range(2):
            for col in range(columns):
                summed = lax.dot_general(
                    select,
                    acc[r, col].reshape(nv * 8, nxy),
                    (((1,), (1,)), ((), ())),
                    precision=HIGHEST,
                    preferred_element_type=F32,
                )
                out = jnp.dot(summed, hit, precision=HIGHEST, preferred_element_type=F32)
                rhs[r, col] = out
                first[r, col] = RELAX_WEIGHT * out


CHUNK = 3


def null_spec(null):
    columns, _, nv, comps, rows, nxy = null.shape
    return pl.BlockSpec((columns, 2, CHUNK, comps, rows, nxy), lambda i: (0, 0, i, 0, 0, 0))


def restrict(slot, partial, gauge, null, halos):
    columns, _, nv, comps, rows, nxy = null.shape
    cy = LY // BLK
    coarse = near_like((2, columns, cy, nv))
    return pl.pallas_call(
        restrict_kernel,
        grid=(nv // CHUNK,),
        in_specs=[pl.BlockSpec(memory_space=SMEM), whole(None), whole(None), null_spec(null)]
        + [whole(h) for h in halos],
        out_specs=[whole(None)] * 3,
        out_shape=[near_like(partial.shape), coarse, coarse],
        scratch_shapes=[
            pltpu.VMEM((columns, 2, comps, rows, nxy), F32),
            pltpu.VMEM((2, columns, nv, 8, nxy), F32),
        ],
        name="restrict",
        compiler_params=pltpu.CompilerParams(vmem_limit_bytes=24 << 20),
    )(slot, near(partial), near(gauge), null, *[near(h) for h in halos])


def relax_kernel(rhs, w, up_t, down_t, up_z, down_z, up_x, down_x, blocks, out):
    columns, cy, nv = w.shape[1:]
    row = lax.broadcasted_iota(jnp.int32, (nv, cy, nv), 0)
    lane = lax.broadcasted_iota(jnp.int32, (nv, cy, nv), 2)
    for col in range(columns):

        def ring(r, by):
            x = w[r, col]
            if by > 0:
                return jnp.concatenate([x[1:], x[:1]], axis=0)
            return jnp.concatenate([x[-1:], x[:-1]], axis=0)

        around = []
        for r in range(2):
            around.append(
                [
                    w[r, col],
                    up_t[r, col],
                    down_t[r, col],
                    w[r, col + 1] if col < columns - 1 else up_z[r, 0],
                    w[r, col - 1] if col > 0 else down_z[r, columns - 1],
                    up_x[r, col],
                    down_x[r, col],
                    ring(r, 1),
                    ring(r, -1),
                ]
            )
        re = im = None
        for k in range(9):
            br = blocks[k, 0, :, col]
            bi = blocks[k, 1, :, col]
            wr = around[0][k][None]
            wi = around[1][k][None]
            pr = br * wr - bi * wi
            pi = br * wi + bi * wr
            re = pr if re is None else re + pr
            im = pi if im is None else im + pi
        for r, part in enumerate((re, im)):
            total = jnp.sum(part, axis=2, keepdims=True)
            total = jnp.sum(jnp.where(row == lane, total, 0.0), axis=0)
            mine = w[r, col]
            out[r, col] = mine + RELAX_WEIGHT * (rhs[r, col] - (2.0 * mine + total))


def relax(rhs, w, blocks):
    up_t = shifted(w, "ta", -1)
    down_t = shifted(w, "ta", 1)
    up_z = shifted(w, "gz", -1)
    down_z = up_z if lax.axis_size("gz") == 2 else shifted(w, "gz", 1)
    up_x = shifted(w, "xy", -1)
    down_x = shifted(w, "xy", 1)
    args = [near(a) for a in (rhs, w, up_t, down_t, up_z, down_z, up_x, down_x, blocks)]
    return pl.pallas_call(
        relax_kernel,
        grid=(1,),
        in_specs=[whole(a) for a in args],
        out_specs=whole(w),
        out_shape=near_like(w.shape),
        name="relax",
        compiler_params=pltpu.CompilerParams(vmem_limit_bytes=24 << 20),
    )(*args)


def prolong_kernel(
    slot, signs, w, iterate, gauge, null, corr, new, o0, o1, o2, o3, o4, o5, spread, fine
):
    step = pl.program_id(0)
    nt, nz, nxy = corr.shape[3:]
    chunk = null.shape[2]
    columns, cy, nv = w.shape[1:]

    @pl.when(step == 0)
    def _():
        select = cy_select(nxy, cy)
        for r in range(2):
            for col in range(columns):
                exact = w[r, col].astype(jnp.bfloat16).astype(F32)
                spread[r, col] = lax.dot_general(
                    exact, select, (((0,), (0,)), ((), ())), precision=HIGHEST, preferred_element_type=F32
                )
        fine[...] = jnp.zeros(fine.shape, F32)

    for col in range(columns):
        here = slot[col]
        wide = [
            [spread[r, col, pl.ds(step * chunk + v, 1)] for r in range(2)] for v in range(chunk)
        ]
        for s in range(12):
            re = fine[col, 0, s]
            im = fine[col, 1, s]
            for v in range(chunk):
                nr = null[here, 0, v, s].astype(F32)
                ni = null[here, 1, v, s].astype(F32)
                wr, wi = wide[v]
                re = re + nr * wr - ni * wi
                im = im + nr * wi + ni * wr
            fine[col, 0, s] = re
            fine[col, 1, s] = im

    @pl.when(step == pl.num_programs(0) - 1)
    def _():
        for r in range(2):
            for s in range(12):
                for t in range(nt):
                    parts = [fine[col, r, s, t * BLK : (t + 1) * BLK] for col in range(columns)]
                    part = jnp.concatenate(parts, axis=0)
                    corr[r, s // 3, s % 3, t] = part
                    new[r, s // 3, s % 3, t] = iterate[r, s // 3, s % 3, t] + part
        write_faces(corr, gauge, edge_signs(signs), (o0, o1, o2, o3, o4, o5))


def prolong(slot, signs, w, iterate, gauge, null):
    columns, _, nv, comps, rows, nxy = null.shape
    shapes = face_shapes(iterate)
    field = jax.ShapeDtypeStruct(iterate.shape, F32)
    out = pl.pallas_call(
        prolong_kernel,
        grid=(nv // CHUNK,),
        in_specs=[pl.BlockSpec(memory_space=SMEM)] * 2 + [whole(None)] * 3 + [null_spec(null)],
        out_specs=[whole(None), full_block(field)] + [whole(s) for s in shapes],
        out_shape=[near_like(iterate.shape), field] + shapes,
        scratch_shapes=[
            pltpu.VMEM((2, columns, nv, nxy), F32),
            pltpu.VMEM((columns, 2, comps, rows, nxy), F32),
        ],
        name="prolong",
        compiler_params=pltpu.CompilerParams(vmem_limit_bytes=24 << 20),
    )(slot, signs, near(w), near(iterate), near(gauge), null)
    return out[0], out[1], out[2:]


def finish_kernel(partial, gauge, h0, h1, h2, h3, h4, h5, res):
    res[...] = partial[...]
    add_halo(res, gauge, (h0, h1, h2, h3, h4, h5))


def finish(partial, gauge, halos):
    return pl.pallas_call(
        finish_kernel,
        grid=(1,),
        in_specs=[whole(partial), gauge_spec(gauge)] + [whole(h) for h in halos],
        out_specs=full_block(partial),
        out_shape=jax.ShapeDtypeStruct(partial.shape, F32),
        name="finish",
        compiler_params=pltpu.CompilerParams(vmem_limit_bytes=24 << 20),
    )(near(partial), near(gauge), *[near(h) for h in halos])


def per_device(source, iterate, gauge_links, clover, bc_sign, null_store, block_slot, coarse_links):
    signs = bc_sign
    nxy = null_store.shape[-1]
    null = null_store.reshape((-1,) + null_store.shape[3:6] + (BLK * BLK, nxy))
    slot = block_slot.reshape(-1)
    kinds, _, nv = coarse_links.shape[:3]
    blocks = jnp.transpose(coarse_links, (0, 1, 2, 4, 5, 6, 7, 3))
    blocks = blocks.reshape((kinds, 2, nv, -1) + blocks.shape[-2:])

    faces = make_faces(signs, iterate, gauge_links)
    halos = swap_faces(faces)
    partial = apply_local(signs, source, iterate, gauge_links, clover)
    residual_start, coarse_rhs, coarse_sol = restrict(slot, partial, gauge_links, null, halos)
    for _ in range(CITERS - 1):
        coarse_sol = relax(coarse_rhs, coarse_sol, blocks)
    correction, new_iterate, faces = prolong(
        slot, signs, coarse_sol, iterate, gauge_links, null
    )
    halos = swap_faces(faces)
    partial = apply_local(signs, residual_start, correction, gauge_links, clover)
    new_residual = finish(partial, gauge_links, halos)
    return (new_iterate, new_residual)


def solution(mesh):
    placed = (
        P(None, None, None, "ta", "gz", "xy"),
        P(None, None, None, "ta", "gz", "xy"),
        P(None, None, None, None, "ta", "gz", "xy"),
        P(None, None, None, None, "ta", "gz", "xy"),
        P(),
        P("ta", "gz", "xy", None, None, None, None, None, None),
        P("ta", "gz", "xy"),
        P(None, None, None, None, "ta", "gz", "xy", None),
    )
    return jax.shard_map(
        per_device,
        mesh=mesh,
        in_specs=placed,
        out_specs=(P(None, None, None, "ta", "gz", "xy"), P(None, None, None, "ta", "gz", "xy")),
        check_vma=False,
    )
```

```python
import jax
import jax.numpy as jnp
from jax import lax
from jax.experimental import pallas as pl
from jax.experimental.pallas import tpu as pltpu
from jax.sharding import PartitionSpec as P

BLK = 4
LY = 32
CITERS = 4
MASS_TERM = 3.8
RELAX_WEIGHT = 0.4
HIGHEST = lax.Precision.HIGHEST
F32 = jnp.float32
VMEM = pltpu.MemorySpace.VMEM
SMEM = pltpu.MemorySpace.SMEM


def times_i(z, sign):
    return (-z[1], z[0]) if sign > 0 else (z[1], -z[0])


def add(a, b):
    return (a[0] + b[0], a[1] + b[1])


def neg(a):
    return (-a[0], -a[1])


def upper_of(mu, low):
    if mu == 0:
        return [low[0], low[1]]
    if mu == 1:
        return [times_i(low[0], -1), times_i(low[1], 1)]
    if mu == 2:
        return [times_i(low[1], -1), times_i(low[0], -1)]
    return [neg(low[1]), low[0]]


def lower_of(mu, half):
    if mu == 0:
        return [half[0], half[1]]
    if mu == 1:
        return [times_i(half[0], 1), times_i(half[1], -1)]
    if mu == 2:
        return [times_i(half[1], 1), times_i(half[0], 1)]
    return [half[1], neg(half[0])]


def project(mu, sign, v):
    out = []
    for c in range(3):
        up = upper_of(mu, [v[2][c], v[3][c]])
        out.append([add(v[s][c], up[s] if sign > 0 else neg(up[s])) for s in range(2)])
    return [[out[c][s] for c in range(3)] for s in range(2)]


def reconstruct(mu, sign, half):
    low = [[None] * 3, [None] * 3]
    for c in range(3):
        lo = lower_of(mu, [half[0][c], half[1][c]])
        for s in range(2):
            low[s][c] = lo[s] if sign > 0 else neg(lo[s])
    return [half[0], half[1], low[0], low[1]]


def link_times(u, half):
    out = []
    for s in range(2):
        row = []
        for a in range(3):
            re = im = None
            for b in range(3):
                ur, ui = u[a][b]
                hr, hi = half[s][b]
                pr = ur * hr - ui * hi
                pi = ur * hi + ui * hr
                re = pr if re is None else re + pr
                im = pi if im is None else im + pi
            row.append((re, im))
        out.append(row)
    return out


def link_dagger(u, half):
    out = []
    for s in range(2):
        row = []
        for a in range(3):
            re = im = None
            for b in range(3):
                ur, ui = u[b][a]
                hr, hi = half[s][b]
                pr = ur * hr + ui * hi
                pi = ur * hi - ui * hr
                re = pr if re is None else re + pr
                im = pi if im is None else im + pi
            row.append((re, im))
        out.append(row)
    return out


def map_half(fn, half):
    return [[(fn(z[0]), fn(z[1])) for z in row] for row in half]


def spinor(get):
    return [[(get(0, s, c), get(1, s, c)) for c in range(3)] for s in range(4)]


def links(get):
    return [[(get(0, a, b), get(1, a, b)) for b in range(3)] for a in range(3)]


def half_of(get):
    return [[(get(0, s, c), get(1, s, c)) for c in range(3)] for s in range(2)]


def put_half(ref, half):
    for s in range(2):
        for c in range(3):
            for r in range(2):
                ref[r, s, c] = half[s][c][r]


def lane_index(shape):
    return lax.broadcasted_iota(jnp.int32, shape, len(shape) - 1)


def edge_signs(bc):
    signs = []
    for i, axis in enumerate(("ta", "gz", "xy")):
        place = lax.axis_index(axis)
        flip = bc[i].astype(F32)
        signs.append(jnp.where(place == 0, flip, 1.0))
        signs.append(jnp.where(place == lax.axis_size(axis) - 1, flip, 1.0))
    return signs


def write_faces(field, gauge, signs, outs):
    to_down_t, to_up_t, to_down_z, to_up_z, to_down_x, to_up_x = outs
    nt, nz, nxy = field.shape[3:]
    half = project(0, -1, spinor(lambda r, s, c: field[r, s, c, 0]))
    put_half(to_down_t, map_half(lambda x: x * signs[0], half))
    half = project(0, 1, spinor(lambda r, s, c: field[r, s, c, nt - 1]))
    half = link_dagger(links(lambda r, a, b: gauge[0, r, a, b, nt - 1]), half)
    put_half(to_up_t, map_half(lambda x: x * signs[1], half))
    half = project(1, -1, spinor(lambda r, s, c: field[r, s, c, :, 0, :]))
    put_half(to_down_z, map_half(lambda x: x * signs[2], half))
    half = project(1, 1, spinor(lambda r, s, c: field[r, s, c, :, nz - 1, :]))
    half = link_dagger(links(lambda r, a, b: gauge[1, r, a, b, :, nz - 1, :]), half)
    put_half(to_up_z, map_half(lambda x: x * signs[3], half))
    lane = lane_index((nz, nxy))

    def packed(rows, first):
        out = None
        for t in range(nt):
            shift = (LY * t - first) % nxy
            x = rows(t)
            x = pltpu.roll(x, shift, 1) if shift else x
            out = x if out is None else jnp.where(lane >= LY * t, x, out)
        return out

    half = project(2, -1, spinor(lambda r, s, c: packed(lambda t: field[r, s, c, t], 0)))
    put_half(to_down_x, map_half(lambda x: x * signs[4], half))
    last = nxy - LY
    half = project(2, 1, spinor(lambda r, s, c: packed(lambda t: field[r, s, c, t], last)))
    half = link_dagger(
        links(lambda r, a, b: packed(lambda t: gauge[2, r, a, b, t], last)), half
    )
    put_half(to_up_x, map_half(lambda x: x * signs[5], half))


def add_halo(res, gauge, halos):
    from_up_t, from_down_t, from_up_z, from_down_z, from_up_x, from_down_x = halos
    nt, nz, nxy = res.shape[3:]

    def accumulate(full, index):
        for s in range(4):
            for c in range(3):
                for r in range(2):
                    where = (r, s, c) + index
                    res[where] = res[where] + 0.5 * full[s][c][r]

    half = half_of(lambda r, s, c: from_up_t[r, s, c])
    half = link_times(links(lambda r, a, b: gauge[0, r, a, b, nt - 1]), half)
    accumulate(reconstruct(0, -1, half), (nt - 1,))
    half = half_of(lambda r, s, c: from_down_t[r, s, c])
    accumulate(reconstruct(0, 1, half), (0,))
    every = slice(None)
    half = half_of(lambda r, s, c: from_up_z[r, s, c])
    half = link_times(links(lambda r, a, b: gauge[1, r, a, b, :, nz - 1, :]), half)
    accumulate(reconstruct(1, -1, half), (every, nz - 1, every))
    half = half_of(lambda r, s, c: from_down_z[r, s, c])
    accumulate(reconstruct(1, 1, half), (every, 0, every))
    lane = lane_index((nz, nxy))
    last = nxy - LY
    for t in range(nt):

        def unpacked(x, first):
            shift = (first - LY * t) % nxy
            x = pltpu.roll(x, shift, 1) if shift else x
            return jnp.where((lane >= first) & (lane < first + LY), x, 0.0)

        half = half_of(lambda r, s, c: unpacked(from_up_x[r, s, c], last))
        half = link_times(links(lambda r, a, b: gauge[2, r, a, b, t]), half)
        accumulate(reconstruct(2, -1, half), (t,))
        half = half_of(lambda r, s, c: unpacked(from_down_x[r, s, c], 0))
        accumulate(reconstruct(2, 1, half), (t,))


def local_kernel(signs, base, field, gauge, *rest):
    t = pl.program_id(0)
    clover, out = rest[-2:]
    streamed = len(rest) == 3
    here = 0 if streamed else t
    nt, nz, nxy = field.shape[3:]
    lane = lane_index((nz, nxy))
    depth = lax.broadcasted_iota(jnp.int32, (nz, nxy), 0)
    y = lane % LY
    v = spinor(lambda r, s, c: field[r, s, c, t])
    hops = [[[None, None] for _ in range(3)] for _ in range(4)]

    def gather(full):
        for s in range(4):
            for c in range(3):
                for r in range(2):
                    old = hops[s][c][r]
                    hops[s][c][r] = full[s][c][r] if old is None else old + full[s][c][r]

    up = jnp.minimum(t + 1, nt - 1)
    down = jnp.maximum(t - 1, 0)
    keep_up = jnp.where(t < nt - 1, 1.0, 0.0).astype(F32)
    keep_down = jnp.where(t > 0, 1.0, 0.0).astype(F32)
    half = project(0, -1, spinor(lambda r, s, c: field[r, s, c, up]))
    half = map_half(lambda x: x * keep_up, half)
    half = link_times(links(lambda r, a, b: gauge[0, r, a, b, here]), half)
    gather(reconstruct(0, -1, half))

    def before_t(r, a, b):
        return rest[0][0, r, a, b, 0] if streamed else gauge[0, r, a, b, down]

    half = project(0, 1, spinor(lambda r, s, c: field[r, s, c, down]))
    half = map_half(lambda x: x * keep_down, half)
    half = link_dagger(links(before_t), half)
    gather(reconstruct(0, 1, half))

    sign_y = signs[3].astype(F32)
    ahead_y = jnp.where(y == LY - 1, sign_y, 1.0)
    behind_y = jnp.where(y == 0, sign_y, 1.0)
    shifts = {
        1: (
            lambda x: jnp.where(depth < nz - 1, pltpu.roll(x, nz - 1, 0), 0.0),
            lambda x: jnp.where(depth > 0, pltpu.roll(x, 1, 0), 0.0),
        ),
        2: (
            lambda x: jnp.where(lane < nxy - LY, pltpu.roll(x, nxy - LY, 1), 0.0),
            lambda x: jnp.where(lane >= LY, pltpu.roll(x, LY, 1), 0.0),
        ),
        3: (
            lambda x: ahead_y
            * jnp.where(y == LY - 1, pltpu.roll(x, LY - 1, 1), pltpu.roll(x, nxy - 1, 1)),
            lambda x: behind_y
            * jnp.where(y == 0, pltpu.roll(x, nxy + 1 - LY, 1), pltpu.roll(x, 1, 1)),
        ),
    }
    for mu in (1, 2, 3):
        u = links(lambda r, a, b: gauge[mu, r, a, b, here])
        half = map_half(shifts[mu][0], project(mu, -1, v))
        gather(reconstruct(mu, -1, link_times(u, half)))
        half = map_half(shifts[mu][1], link_dagger(u, project(mu, 1, v)))
        gather(reconstruct(mu, 1, half))

    for chi in range(2):
        for a in range(6):
            s, c = 2 * chi + a // 3, a % 3
            re = MASS_TERM * v[s][c][0] - 0.5 * hops[s][c][0]
            im = MASS_TERM * v[s][c][1] - 0.5 * hops[s][c][1]
            for b in range(6):
                vr, vi = v[2 * chi + b // 3][b % 3]
                cr = clover[chi, 0, a, b, here]
                ci = clover[chi, 1, a, b, here]
                re = re + cr * vr - ci * vi
                im = im + cr * vi + ci * vr
            out[0, s, c, t] = base[0, s, c, here] - re
            out[1, s, c, t] = base[1, s, c, here] - im


def apply_local(signs, base, field, gauge, clover):
    return pl.pallas_call(
        local_kernel,
        grid=(field.shape[3],),
        in_specs=[pl.BlockSpec(memory_space=SMEM)] + [whole(None)] * 4,
        out_specs=whole(None),
        out_shape=near_like(field.shape),
        cost_estimate=pl.CostEstimate(flops=12_000_000, transcendentals=0, bytes_accessed=5_000_000),
        name="local_part",
        compiler_params=pltpu.CompilerParams(vmem_limit_bytes=24 << 20),
    )(signs, near(base), near(field), near(gauge), near(clover))


def apply_streamed(signs, base, field, gauge, clover):
    nt, nz, nxy = field.shape[3:]
    slice_of = lambda shape: pl.BlockSpec(shape, lambda t: (0,) * (len(shape) - 3) + (t, 0, 0))
    return pl.pallas_call(
        local_kernel,
        grid=(nt,),
        in_specs=[
            pl.BlockSpec(memory_space=SMEM),
            slice_of((2, 4, 3, 1, nz, nxy)),
            full_block(field),
            slice_of((4, 2, 3, 3, 1, nz, nxy)),
            pl.BlockSpec(
                (1, 2, 3, 3, 1, nz, nxy), lambda t: (0, 0, 0, 0, jnp.maximum(t - 1, 0), 0, 0)
            ),
            slice_of((2, 2, 6, 6, 1, nz, nxy)),
        ],
        out_specs=whole(None),
        out_shape=near_like(field.shape),
        cost_estimate=pl.CostEstimate(flops=12_000_000, transcendentals=0, bytes_accessed=5_000_000),
        name="local_streamed",
        compiler_params=pltpu.CompilerParams(vmem_limit_bytes=24 << 20),
    )(signs, far(base), far(field), far(gauge), far(gauge), far(clover))


def face_shapes(field):
    nt, nz, nxy = field.shape[3:]
    row = near_like((2, 2, 3, nz, nxy))
    slab = near_like((2, 2, 3, nt, nxy))
    return [row, row, slab, slab, row, row]


def faces_kernel(signs, field, gauge, *outs):
    write_faces(field, gauge, edge_signs(signs), outs)


def whole(x):
    return pl.BlockSpec(memory_space=VMEM)


def gauge_spec(gauge):
    return full_block(jax.ShapeDtypeStruct((3,) + gauge.shape[1:], gauge.dtype))


def full_block(x):
    n = len(x.shape)
    return pl.BlockSpec(x.shape, lambda *_: (0,) * n)


def near(x):
    return pltpu.with_memory_space_constraint(x, VMEM)


def far(x):
    return pltpu.with_memory_space_constraint(x, pltpu.MemorySpace.HBM)


def near_like(shape):
    return VMEM(tuple(shape), F32)


def make_faces(signs, field, gauge):
    shapes = face_shapes(field)
    return pl.pallas_call(
        faces_kernel,
        grid=(1,),
        in_specs=[pl.BlockSpec(memory_space=SMEM), full_block(field), gauge_spec(gauge)],
        out_specs=[whole(s) for s in shapes],
        out_shape=shapes,
        name="faces",
        compiler_params=pltpu.CompilerParams(vmem_limit_bytes=24 << 20),
    )(signs, far(field), far(gauge))


def shifted(value, axis, by):
    n = lax.axis_size(axis)
    return lax.ppermute(value, axis, [(i, (i + by) % n) for i in range(n)])


def swap_faces(faces):
    out = []
    for i, axis in enumerate(("ta", "gz", "xy")):
        out.append(shifted(faces[2 * i], axis, -1))
        out.append(shifted(faces[2 * i + 1], axis, 1))
    return out


def cy_select(nxy, cy):
    lane = lax.broadcasted_iota(jnp.int32, (cy, nxy), 1)
    row = lax.broadcasted_iota(jnp.int32, (cy, nxy), 0)
    return jnp.where((lane % LY) // BLK == row, 1.0, 0.0).astype(F32)


def restrict_kernel(slot, partial, gauge, null, h0, h1, h2, h3, h4, h5, res, rhs, first, rounded, acc):
    step = pl.program_id(0)
    nt, nz, nxy = res.shape[3:]
    chunk = null.shape[2]
    nv = acc.shape[2]
    columns, cy = rhs.shape[1:3]

    rows = nt * BLK

    @pl.when(step == 0)
    def _():
        res[...] = partial[...]
        add_halo(res, gauge, (h0, h1, h2, h3, h4, h5))
        for r in range(2):
            for s in range(12):
                for col in range(columns):
                    parts = [
                        res[r, s // 3, s % 3, t, col * BLK : (col + 1) * BLK] for t in range(nt)
                    ]
                    part = jnp.concatenate(parts, axis=0)
                    rounded[col, r, s] = part.astype(jnp.bfloat16).astype(F32)

    for col in range(columns):
        here = slot[col]
        res_re = [jnp.zeros((rows, nxy), F32) for _ in range(chunk)]
        res_im = [jnp.zeros((rows, nxy), F32) for _ in range(chunk)]
        for s in range(12):
            fr = rounded[col, 0, s]
            fi = rounded[col, 1, s]
            for v in range(chunk):
                nr = null[here, 0, v, s].astype(F32)
                ni = null[here, 1, v, s].astype(F32)
                res_re[v] = res_re[v] + nr * fr + ni * fi
                res_im[v] = res_im[v] + nr * fi - ni * fr
        for v in range(chunk):
            for r, part in enumerate((res_re[v], res_im[v])):
                total = part[0:8]
                for first_row in range(8, rows, 8):
                    total = total + part[first_row : first_row + 8]
                acc[r, col, step * chunk + v] = total

    @pl.when(step == pl.num_programs(0) - 1)
    def _():
        select = cy_select(nxy, cy)
        from_row = lax.broadcasted_iota(jnp.int32, (nv * 8, nv), 0)
        to_lane = lax.broadcasted_iota(jnp.int32, (nv * 8, nv), 1)
        hit = jnp.where(from_row // 8 == to_lane, 1.0, 0.0).astype(F32)
        for r in range(2):
            for col in range(columns):
                summed = lax.dot_general(
                    select,
                    acc[r, col].reshape(nv * 8, nxy),
                    (((1,), (1,)), ((), ())),
                    precision=HIGHEST,
                    preferred_element_type=F32,
                )
                out = jnp.dot(summed, hit, precision=HIGHEST, preferred_element_type=F32)
                rhs[r, col] = out
                first[r, col] = RELAX_WEIGHT * out


CHUNK = 3


def null_spec(null):
    columns, _, nv, comps, rows, nxy = null.shape
    return pl.BlockSpec((columns, 2, CHUNK, comps, rows, nxy), lambda i: (0, 0, i, 0, 0, 0))


def restrict(slot, partial, gauge, null, halos):
    columns, _, nv, comps, rows, nxy = null.shape
    cy = LY // BLK
    coarse = near_like((2, columns, cy, nv))
    return pl.pallas_call(
        restrict_kernel,
        grid=(nv // CHUNK,),
        in_specs=[pl.BlockSpec(memory_space=SMEM), whole(None), whole(None), null_spec(null)]
        + [whole(h) for h in halos],
        out_specs=[whole(None)] * 3,
        out_shape=[near_like(partial.shape), coarse, coarse],
        scratch_shapes=[
            pltpu.VMEM((columns, 2, comps, rows, nxy), F32),
            pltpu.VMEM((2, columns, nv, 8, nxy), F32),
        ],
        name="restrict",
        compiler_params=pltpu.CompilerParams(vmem_limit_bytes=24 << 20),
    )(slot, near(partial), near(gauge), null, *[near(h) for h in halos])


def relax_kernel(rhs, w, up_t, down_t, up_z, down_z, up_x, down_x, blocks, out):
    columns, cy, nv = w.shape[1:]
    row = lax.broadcasted_iota(jnp.int32, (nv, cy, nv), 0)
    lane = lax.broadcasted_iota(jnp.int32, (nv, cy, nv), 2)
    for col in range(columns):

        def ring(r, by):
            x = w[r, col]
            if by > 0:
                return jnp.concatenate([x[1:], x[:1]], axis=0)
            return jnp.concatenate([x[-1:], x[:-1]], axis=0)

        around = []
        for r in range(2):
            around.append(
                [
                    w[r, col],
                    up_t[r, col],
                    down_t[r, col],
                    w[r, col + 1] if col < columns - 1 else up_z[r, 0],
                    w[r, col - 1] if col > 0 else down_z[r, columns - 1],
                    up_x[r, col],
                    down_x[r, col],
                    ring(r, 1),
                    ring(r, -1),
                ]
            )
        re = im = None
        for k in range(9):
            br = blocks[k, 0, :, col]
            bi = blocks[k, 1, :, col]
            wr = around[0][k][None]
            wi = around[1][k][None]
            pr = br * wr - bi * wi
            pi = br * wi + bi * wr
            re = pr if re is None else re + pr
            im = pi if im is None else im + pi
        for r, part in enumerate((re, im)):
            total = jnp.sum(part, axis=2, keepdims=True)
            total = jnp.sum(jnp.where(row == lane, total, 0.0), axis=0)
            mine = w[r, col]
            out[r, col] = mine + RELAX_WEIGHT * (rhs[r, col] - (2.0 * mine + total))


def relax(rhs, w, blocks):
    up_t = shifted(w, "ta", -1)
    down_t = shifted(w, "ta", 1)
    up_z = shifted(w, "gz", -1)
    down_z = up_z if lax.axis_size("gz") == 2 else shifted(w, "gz", 1)
    up_x = shifted(w, "xy", -1)
    down_x = shifted(w, "xy", 1)
    args = [near(a) for a in (rhs, w, up_t, down_t, up_z, down_z, up_x, down_x, blocks)]
    return pl.pallas_call(
        relax_kernel,
        grid=(1,),
        in_specs=[whole(a) for a in args],
        out_specs=whole(w),
        out_shape=near_like(w.shape),
        name="relax",
        compiler_params=pltpu.CompilerParams(vmem_limit_bytes=24 << 20),
    )(*args)


def prolong_kernel(
    slot, signs, w, iterate, gauge, null, corr, new, o0, o1, o2, o3, o4, o5, spread, fine
):
    step = pl.program_id(0)
    nt, nz, nxy = corr.shape[3:]
    chunk = null.shape[2]
    columns, cy, nv = w.shape[1:]

    @pl.when(step == 0)
    def _():
        select = cy_select(nxy, cy)
        for r in range(2):
            for col in range(columns):
                exact = w[r, col].astype(jnp.bfloat16).astype(F32)
                spread[r, col] = lax.dot_general(
                    exact, select, (((0,), (0,)), ((), ())), precision=HIGHEST, preferred_element_type=F32
                )
        fine[...] = jnp.zeros(fine.shape, F32)

    for col in range(columns):
        here = slot[col]
        wide = [
            [spread[r, col, pl.ds(step * chunk + v, 1)] for r in range(2)] for v in range(chunk)
        ]
        for s in range(12):
            re = fine[col, 0, s]
            im = fine[col, 1, s]
            for v in range(chunk):
                nr = null[here, 0, v, s].astype(F32)
                ni = null[here, 1, v, s].astype(F32)
                wr, wi = wide[v]
                re = re + nr * wr - ni * wi
                im = im + nr * wi + ni * wr
            fine[col, 0, s] = re
            fine[col, 1, s] = im

    @pl.when(step == pl.num_programs(0) - 1)
    def _():
        for r in range(2):
            for s in range(12):
                for t in range(nt):
                    parts = [fine[col, r, s, t * BLK : (t + 1) * BLK] for col in range(columns)]
                    part = jnp.concatenate(parts, axis=0)
                    corr[r, s // 3, s % 3, t] = part
                    new[r, s // 3, s % 3, t] = iterate[r, s // 3, s % 3, t] + part
        write_faces(corr, gauge, edge_signs(signs), (o0, o1, o2, o3, o4, o5))


def prolong(slot, signs, w, iterate, gauge, null):
    columns, _, nv, comps, rows, nxy = null.shape
    shapes = face_shapes(iterate)
    field = jax.ShapeDtypeStruct(iterate.shape, F32)
    out = pl.pallas_call(
        prolong_kernel,
        grid=(nv // CHUNK,),
        in_specs=[pl.BlockSpec(memory_space=SMEM)] * 2 + [whole(None)] * 3 + [null_spec(null)],
        out_specs=[whole(None), full_block(field)] + [whole(s) for s in shapes],
        out_shape=[near_like(iterate.shape), field] + shapes,
        scratch_shapes=[
            pltpu.VMEM((2, columns, nv, nxy), F32),
            pltpu.VMEM((columns, 2, comps, rows, nxy), F32),
        ],
        name="prolong",
        compiler_params=pltpu.CompilerParams(vmem_limit_bytes=24 << 20),
    )(slot, signs, near(w), near(iterate), near(gauge), null)
    return out[0], out[1], out[2:]


def finish_kernel(partial, gauge, h0, h1, h2, h3, h4, h5, res):
    res[...] = partial[...]
    add_halo(res, gauge, (h0, h1, h2, h3, h4, h5))


def finish(partial, gauge, halos):
    return pl.pallas_call(
        finish_kernel,
        grid=(1,),
        in_specs=[whole(partial), whole(gauge)] + [whole(h) for h in halos],
        out_specs=full_block(partial),
        out_shape=jax.ShapeDtypeStruct(partial.shape, F32),
        name="finish",
        compiler_params=pltpu.CompilerParams(vmem_limit_bytes=24 << 20),
    )(near(partial), near(gauge), *[near(h) for h in halos])


def per_device(source, iterate, gauge_links, clover, bc_sign, null_store, block_slot, coarse_links):
    signs = bc_sign
    nxy = null_store.shape[-1]
    null = null_store.reshape((-1,) + null_store.shape[3:6] + (BLK * BLK, nxy))
    slot = block_slot.reshape(-1)
    kinds, _, nv = coarse_links.shape[:3]
    blocks = jnp.transpose(coarse_links, (0, 1, 2, 4, 5, 6, 7, 3))
    blocks = blocks.reshape((kinds, 2, nv, -1) + blocks.shape[-2:])

    faces = make_faces(signs, iterate, gauge_links)
    halos = swap_faces(faces)
    partial = apply_streamed(signs, source, iterate, gauge_links, clover)
    residual_start, coarse_rhs, coarse_sol = restrict(slot, partial, gauge_links, null, halos)
    for _ in range(CITERS - 1):
        coarse_sol = relax(coarse_rhs, coarse_sol, blocks)
    correction, new_iterate, faces = prolong(
        slot, signs, coarse_sol, iterate, gauge_links, null
    )
    halos = swap_faces(faces)
    partial = apply_local(signs, residual_start, correction, gauge_links, clover)
    new_residual = finish(partial, gauge_links, halos)
    return (new_iterate, new_residual)


def solution(mesh):
    placed = (
        P(None, None, None, "ta", "gz", "xy"),
        P(None, None, None, "ta", "gz", "xy"),
        P(None, None, None, None, "ta", "gz", "xy"),
        P(None, None, None, None, "ta", "gz", "xy"),
        P(),
        P("ta", "gz", "xy", None, None, None, None, None, None),
        P("ta", "gz", "xy"),
        P(None, None, None, None, "ta", "gz", "xy", None),
    )
    return jax.shard_map(
        per_device,
        mesh=mesh,
        in_specs=placed,
        out_specs=(P(None, None, None, "ta", "gz", "xy"), P(None, None, None, "ta", "gz", "xy")),
        check_vma=False,
    )
```
